32 devices in a mesh: gx: 4 (over z), gy: 4 (over x, core), gz: 2 (over y).
Axes of the slice: x: 2, y: 2, z: 4, core: 2. Of those that a mesh axis runs over, the one named last changes fastest.
Arguments:
- right_side: bfloat16 [16, 256, 512], P('gz', 'gx', 'gy'), may hold values from -6 to 6
- phase_mask: int32 [16, 256, 512], P('gz', 'gx', 'gy'), may hold values from 0 to 1, as said below
Outputs:
- pressure: float32 [16, 256, 512], P('gz', 'gx', 'gy')
- scaled_residual: float32 [16, 256, 512], P('gz', 'gx', 'gy')
The draws below stay inside these ranges and needn't reach their ends.
Inputs may be any that keep to these rules, and one draw needn't show every extreme that they name: `phase_mask`: 0 for a gas cell, 1 for a liquid cell.
All inputs are finite; a program needn't handle non-finite values.
Results may differ from the reference program's by a relative error of at most 0.0004.
Values may be sent and summed in bfloat16 or wider, within the bound.
A program may use at most 64 MiB of HBM per device.

```python
import math
import jax
import jax.numpy as jnp

ITERS = 3
NZ = 16
NX = 256
NY = 512


def draw_right_side(key, part):
    k_noise, k_phase, k_amp = jax.random.split(jax.random.fold_in(key, 11), 3)
    zpos = jnp.arange(NZ, dtype=jnp.float32)[:, None, None] / NZ
    xpos = jnp.arange(NX, dtype=jnp.float32)[None, :, None] / NX
    ypos = jnp.arange(NY, dtype=jnp.float32)[None, None, :] / NY
    phases = jax.random.uniform(k_phase, (4,), jnp.float32, -math.pi, math.pi)
    amps = jax.random.uniform(k_amp, (4,), jnp.float32, 0.5, 1.0)
    turn = 2.0 * math.pi
    smooth = amps[0] * jnp.sin(turn * xpos + phases[0])
    smooth = smooth + amps[1] * jnp.sin(turn * ypos + phases[1])
    smooth = smooth + amps[2] * jnp.sin(turn * zpos + phases[2])
    smooth = smooth + amps[3] * jnp.sin(turn * (xpos + ypos) + phases[3])
    noise = jax.random.normal(k_noise, (NZ, NX, NY), jnp.float32)
    return jnp.clip(noise + smooth, -6.0, 6.0).astype(jnp.bfloat16)


def draw_phase_mask(key, part):
    k_low, k_high, k_cell = jax.random.split(jax.random.fold_in(key, 7), 3)
    lower = jax.random.randint(k_low, (), 100, 301, jnp.int32)
    upper = jax.random.randint(k_high, (), 400, 701, jnp.int32)
    zindex = jnp.arange(NZ, dtype=jnp.int32)[:, None, None]
    xindex = jnp.arange(NX, dtype=jnp.int32)[None, :, None]
    ramp = (upper - lower) * (xindex * NZ + zindex * NX) // (2 * NX * NZ)
    threshold = lower + ramp
    cells = jax.random.randint(k_cell, (NZ, NX, NY), 0, 1000, jnp.int32)
    return (cells < threshold).astype(jnp.int32)


def setup_inputs(seed: int = 0) -> dict:
    key_of = jax.random.split(jax.random.key(seed), 3)
    right_side = draw_right_side(jax.random.fold_in(key_of[2], 71), 0)
    phase_mask = draw_phase_mask(jax.random.fold_in(key_of[2], 71), 0)
    return dict(right_side=right_side, phase_mask=phase_mask)


density_ratio = 1000.0
mass_shift = 0.05


def coupling(density, axis, offset):
    return 2.0 / (density + jnp.roll(density, offset, axis))


def operate(field, density):
    total = mass_shift * field
    for axis in range(3):
        for offset in (1, -1):
            total = total + coupling(density, axis, offset) * (field - jnp.roll(field, offset, axis))
    return total


def reference(right_side, phase_mask):
    density = 1.0 + (density_ratio - 1.0) * phase_mask.astype(jnp.float32)
    diagonal = jnp.full(density.shape, mass_shift, jnp.float32)
    for axis in range(3):
        for offset in (1, -1):
            diagonal = diagonal + coupling(density, axis, offset)
    source = diagonal * right_side.astype(jnp.float32)
    pressure = jnp.zeros_like(source)
    residual = source
    smoothed = residual / diagonal
    direction = smoothed
    energy = jnp.sum(residual * smoothed)
    for iteration in range(ITERS):
        applied = operate(direction, density)
        step_size = energy / jnp.sum(direction * applied)
        pressure = pressure + step_size * direction
        residual = residual - step_size * applied
        smoothed = residual / diagonal
        energy_next = jnp.sum(residual * smoothed)
        direction = smoothed + (energy_next / energy) * direction
        energy = energy_next
    return pressure, residual / diagonal
```

```python
import functools
import itertools

import jax
import jax.numpy as jnp
from jax import lax
from jax.experimental import pallas as pl
from jax.experimental.pallas import tpu as pltpu
from jax.sharding import PartitionSpec as P

ITERS = 3
AXES = ("gx", "gy", "gz")
MESH = pl.DeviceIdType.MESH
F32 = jnp.float32

density_gas = 1.0
density_liquid = 1000.0
mass_shift = 0.05


def shifted(sizes, offsets):
    return {
        axis: lax.rem(lax.axis_index(axis) + offset, sizes[axis])
        for axis, offset in offsets.items()
        if offset
    }


def group_offsets(sizes, group):
    spans = [range(sizes[axis]) for axis in group]
    return [dict(zip(group, point)) for point in itertools.product(*spans) if any(point)]


def exchange(sizes, phase, faces, landings, send_sems, recv_sems):
    copies = []
    for place, (axis, (low, high), (from_below, from_above)) in enumerate(
        zip(("gz", "gx", "gy"), faces, landings)
    ):
        for side, source, target, offset in (
            (0, high, from_below, 1),
            (1, low, from_above, sizes[axis] - 1),
        ):
            copy = pltpu.make_async_remote_copy(
                src_ref=source,
                dst_ref=target,
                send_sem=send_sems.at[phase, 2 * place + side],
                recv_sem=recv_sems.at[phase, 2 * place + side],
                device_id=shifted(sizes, {axis: offset}),
                device_id_type=MESH,
            )
            copy.start()
            copies.append(copy)
    return copies


def polynomial_sum(first, second, factor):
    length = max(len(first), len(second))
    out = []
    for i in range(length):
        if i >= len(second):
            out.append(first[i])
        elif i >= len(first):
            out.append(factor * second[i])
        else:
            out.append(first[i] + factor * second[i])
    return out


def gradient_coefficients(moments):
    one, zero = jnp.ones_like(moments[0]), jnp.zeros_like(moments[0])

    def inner(first, second, weights):
        total = None
        for i, a in enumerate(first):
            for j, b in enumerate(second):
                term = a * b * weights[i + j]
                total = term if total is None else total + term
        return total

    drops = [moments[i] - moments[i + 1] for i in range(len(moments) - 1)]
    residual, direction, pressure = [one], [one], []
    energy = moments[0]
    for iteration in range(ITERS):
        step = energy / inner(direction, direction, drops)
        pressure = polynomial_sum(pressure, direction, step)
        image = polynomial_sum(direction, [zero] + direction, -1.0)
        residual = polynomial_sum(residual, image, -step)
        if iteration + 1 < ITERS:
            fresh = inner(residual, residual, moments)
            direction = polynomial_sum(residual, direction, fresh / energy)
            energy = fresh
    return pressure, residual


def kernel(
    sizes, groups, right_ref, mask_ref, pressure_ref, scaled_ref,
    fields, phases, coefs, diag, sz0, sx0, rz0, rx0, sx, sy, rz, rx, ry,
    partial, gathered, send_sems, recv_sems, sum_send, sum_recv,
):
    depth, rows, lanes = right_ref.shape
    peers = []
    for offset in [dict([(a, o)]) for a in AXES for o in (1, sizes[a] - 1)] + [
        o for group in groups for o in group_offsets(sizes, group)
    ]:
        if offset not in peers:
            peers.append(offset)
    barrier = pltpu.get_barrier_semaphore()
    for offset in peers:
        pl.semaphore_signal(barrier, inc=1, device_id=shifted(sizes, offset), device_id_type=MESH)

    row = lax.broadcasted_iota(jnp.int32, (rows, lanes), 0)
    lane = lax.broadcasted_iota(jnp.int32, (rows, lanes), 1)
    even = lane % 2 == 0

    def pack(packed, plane, z, base):
        at = base + 2 * z
        turned = pltpu.roll(plane, (at + 1) % lanes, 1)
        return jnp.where((lane == at) | (lane == at + 1), turned, packed)

    def unpack(below, above):
        return jnp.where(even, pltpu.roll(above, lanes - 1, 1), pltpu.roll(below, 1, 1))

    def neighbours(plane, under, over, low_row, high_row, sides, z, base):
        at = base + 2 * z
        edge = pltpu.roll(sides, (lanes - at - 1) % lanes, 1)
        return (
            under,
            over,
            jnp.where(row == 0, low_row, pltpu.roll(plane, 1, 0)),
            jnp.where(row == rows - 1, high_row, pltpu.roll(plane, rows - 1, 0)),
            jnp.where(lane == 0, edge, pltpu.roll(plane, 1, 1)),
            jnp.where(lane == lanes - 1, edge, pltpu.roll(plane, lanes - 1, 1)),
        )

    packed = jnp.zeros((rows, lanes), F32)
    for z in range(depth):
        value = right_ref[z].astype(F32)
        phase = mask_ref[z].astype(F32)
        fields[0, z] = value
        phases[z] = phase
        packed = pack(packed, value, z, 0)
        packed = pack(packed, phase, z, 2 * depth)
        for part, plane in enumerate((value, phase)):
            sx0[0, part, z : z + 1, :] = plane[0:1]
            sx0[1, part, z : z + 1, :] = plane[rows - 1 : rows]
        for side, face in ((0, 0), (1, depth - 1)):
            if z == face:
                sz0[side, 0] = right_ref[z]
                sz0[side, 1] = phase.astype(jnp.bfloat16)
    sy[0] = packed
    pl.semaphore_wait(barrier, len(peers))

    copies = exchange(
        sizes,
        0,
        ((sz0.at[0], sz0.at[1]), (sx0.at[0], sx0.at[1]), (sy.at[0], sy.at[0])),
        ((rz0.at[0], rz0.at[1]), (rx0.at[0], rx0.at[1]), (ry.at[0, 0], ry.at[0, 1])),
        send_sems,
        recv_sems,
    )
    for copy in copies:
        copy.wait()

    def fold(product):
        return jnp.sum(product.reshape(rows // 8, 8, lanes), axis=0)

    sums = [jnp.zeros((8, lanes), F32) for _ in range(2 * ITERS)]
    mixed = 2.0 / (density_gas + density_liquid)
    for phase in range(ITERS):
        sides = unpack(ry[phase, 0], ry[phase, 1])
        packed = jnp.zeros((rows, lanes), F32)
        for z in range(depth):
            if phase == 0:
                below = rz0[0, 1].astype(F32) if z == 0 else phases[z - 1]
                above = rz0[1, 1].astype(F32) if z == depth - 1 else phases[z + 1]
                own = phases[z]
                around = neighbours(
                    own, below, above,
                    rx0[0, 1, z : z + 1, :], rx0[1, 1, z : z + 1, :], sides, z, 2 * depth,
                )
                weights = []
                diagonal = jnp.full((rows, lanes), mass_shift, F32)
                for other in around:
                    count = own + other
                    weight = jnp.where(
                        count < 0.5,
                        1.0 / density_gas,
                        jnp.where(count < 1.5, mixed, 1.0 / density_liquid),
                    )
                    weights.append(weight)
                    diagonal = diagonal + weight
                diag[z] = diagonal
                inverse = 1.0 / diagonal
                weights = [weight * inverse for weight in weights]
                for k, weight in enumerate(weights):
                    coefs[k, z] = weight
                below = rz0[0, 0].astype(F32) if z == 0 else fields[0, z - 1]
                above = rz0[1, 0].astype(F32) if z == depth - 1 else fields[0, z + 1]
                low, high = rx0[0, 0, z : z + 1, :], rx0[1, 0, z : z + 1, :]
            else:
                diagonal = diag[z]
                weights = [coefs[k, z] for k in range(6)]
                below = rz[phase - 1, 0] if z == 0 else fields[phase, z - 1]
                above = rz[phase - 1, 1] if z == depth - 1 else fields[phase, z + 1]
                low, high = rx[phase - 1, 0, z : z + 1, :], rx[phase - 1, 1, z : z + 1, :]
            own = fields[phase, z]
            around = neighbours(own, below, above, low, high, sides, z, 0)
            mean = weights[0] * around[0]
            for weight, other in zip(weights[1:], around[1:]):
                mean = mean + weight * other
            fields[phase + 1, z] = mean
            scaled = diagonal * own
            sums[2 * phase] = sums[2 * phase] + fold(scaled * own)
            sums[2 * phase + 1] = sums[2 * phase + 1] + fold(scaled * mean)
            if phase + 1 < ITERS:
                packed = pack(packed, mean, z, 0)
                sx[phase, 0, z : z + 1, :] = mean[0:1]
                sx[phase, 1, z : z + 1, :] = mean[rows - 1 : rows]
        if phase + 1 < ITERS:
            sy[phase + 1] = packed
            copies = exchange(
                sizes,
                phase + 1,
                (
                    (fields.at[phase + 1, 0], fields.at[phase + 1, depth - 1]),
                    (sx.at[phase, 0], sx.at[phase, 1]),
                    (sy.at[phase + 1], sy.at[phase + 1]),
                ),
                (
                    (rz.at[phase, 0], rz.at[phase, 1]),
                    (rx.at[phase, 0], rx.at[phase, 1]),
                    (ry.at[phase + 1, 0], ry.at[phase + 1, 1]),
                ),
                send_sems,
                recv_sems,
            )
            for copy in copies:
                copy.wait()

    line = lax.broadcasted_iota(jnp.int32, (8, lanes), 0)
    tile = jnp.zeros((8, lanes), F32)
    for k, total in enumerate(sums):
        tile = jnp.where(line == k, jnp.sum(total, axis=0, keepdims=True), tile)
    slot = 0
    for number, group in enumerate(groups):
        partial[number] = tile
        copies = []
        first = slot
        for offset in group_offsets(sizes, group):
            copy = pltpu.make_async_remote_copy(
                src_ref=partial.at[number],
                dst_ref=gathered.at[slot],
                send_sem=sum_send.at[slot],
                recv_sem=sum_recv.at[slot],
                device_id=shifted(sizes, offset),
                device_id_type=MESH,
            )
            copy.start()
            copies.append(copy)
            slot += 1
        for copy in copies:
            copy.wait()
        for k in range(first, slot):
            tile = tile + gathered[k]

    whole = jnp.sum(tile, axis=1, keepdims=True)
    moments = [whole[k : k + 1] for k in range(2 * ITERS)]
    pressure, residual = gradient_coefficients(moments)
    for z in range(depth):
        basis = [fields[k, z] for k in range(ITERS + 1)]
        for ref, factors in ((pressure_ref, pressure), (scaled_ref, residual)):
            total = factors[0] * basis[0]
            for factor, part in zip(factors[1:], basis[1:]):
                total = total + factor * part
            ref[z] = total


def choose_groups(sizes, most=32):
    groups = []
    for axis in ("gz", "gy", "gx"):
        if groups and sizes[axis] * functools.reduce(lambda n, a: n * sizes[a], groups[-1], 1) <= most:
            groups[-1] = groups[-1] + (axis,)
        else:
            groups.append((axis,))
    return tuple(groups)


def solution(mesh):
    sizes = {axis: mesh.shape[axis] for axis in AXES}
    groups = choose_groups(sizes, 8)
    slots = sum(len(group_offsets(sizes, group)) for group in groups)

    def on_device(right_side, phase_mask):
        depth, rows, lanes = right_side.shape
        block = jax.ShapeDtypeStruct((depth, rows, lanes), F32)
        face = (rows, lanes)
        return pl.pallas_call(
            functools.partial(kernel, sizes, groups),
            out_shape=(block, block),
            in_specs=[pl.BlockSpec(memory_space=pltpu.VMEM)] * 2,
            out_specs=(pl.BlockSpec(memory_space=pltpu.VMEM),) * 2,
            scratch_shapes=[
                pltpu.VMEM((ITERS + 1, depth, *face), F32),
                pltpu.VMEM((depth, *face), F32),
                pltpu.VMEM((6, depth, *face), F32),
                pltpu.VMEM((depth, *face), F32),
                pltpu.VMEM((2, 2, *face), jnp.bfloat16),
                pltpu.VMEM((2, 2, depth, lanes), F32),
                pltpu.VMEM((2, 2, *face), jnp.bfloat16),
                pltpu.VMEM((2, 2, depth, lanes), F32),
                pltpu.VMEM((ITERS - 1, 2, depth, lanes), F32),
                pltpu.VMEM((ITERS, *face), F32),
                pltpu.VMEM((ITERS - 1, 2, *face), F32),
                pltpu.VMEM((ITERS - 1, 2, depth, lanes), F32),
                pltpu.VMEM((ITERS, 2, *face), F32),
                pltpu.VMEM((len(groups), 8, lanes), F32),
                pltpu.VMEM((slots, 8, lanes), F32),
                pltpu.SemaphoreType.DMA((ITERS, 6)),
                pltpu.SemaphoreType.DMA((ITERS, 6)),
                pltpu.SemaphoreType.DMA((slots,)),
                pltpu.SemaphoreType.DMA((slots,)),
            ],
            compiler_params=pltpu.CompilerParams(collective_id=0, has_side_effects=True),
        )(right_side, phase_mask)

    return jax.shard_map(
        on_device,
        mesh=mesh,
        in_specs=(P("gz", "gx", "gy"), P("gz", "gx", "gy")),
        out_specs=(P("gz", "gx", "gy"), P("gz", "gx", "gy")),
        check_vma=False,
    )
```

```python
import functools
import itertools

import jax
import jax.numpy as jnp
from jax import lax
from jax.experimental import pallas as pl
from jax.experimental.pallas import tpu as pltpu
from jax.sharding import PartitionSpec as P

ITERS = 3
AXES = ("gx", "gy", "gz")
MESH = pl.DeviceIdType.MESH
F32 = jnp.float32

density_gas = 1.0
density_liquid = 1000.0
mass_shift = 0.05


def shifted(sizes, offsets):
    return {
        axis: lax.rem(lax.axis_index(axis) + offset, sizes[axis])
        for axis, offset in offsets.items()
        if offset
    }


def group_offsets(sizes, group):
    spans = [range(sizes[axis]) for axis in group]
    return [dict(zip(group, point)) for point in itertools.product(*spans) if any(point)]


def exchange(sizes, phase, axis, faces, landings, send_sems, recv_sems):
    place = AXES.index(axis)
    copies = []
    for side, offset in ((0, 1), (1, sizes[axis] - 1)):
        copy = pltpu.make_async_remote_copy(
            src_ref=faces[1 - side],
            dst_ref=landings[side],
            send_sem=send_sems.at[phase, 2 * place + side],
            recv_sem=recv_sems.at[phase, 2 * place + side],
            device_id=shifted(sizes, {axis: offset}),
            device_id_type=MESH,
        )
        copy.start()
        copies.append(copy)
    return copies


def polynomial_sum(first, second, factor):
    length = max(len(first), len(second))
    out = []
    for i in range(length):
        if i >= len(second):
            out.append(first[i])
        elif i >= len(first):
            out.append(factor * second[i])
        else:
            out.append(first[i] + factor * second[i])
    return out


def gradient_coefficients(moments):
    one, zero = jnp.ones_like(moments[0]), jnp.zeros_like(moments[0])

    def inner(first, second, weights):
        total = None
        for i, a in enumerate(first):
            for j, b in enumerate(second):
                term = a * b * weights[i + j]
                total = term if total is None else total + term
        return total

    drops = [moments[i] - moments[i + 1] for i in range(len(moments) - 1)]
    residual, direction, pressure = [one], [one], []
    energy = moments[0]
    for iteration in range(ITERS):
        step = energy / inner(direction, direction, drops)
        pressure = polynomial_sum(pressure, direction, step)
        image = polynomial_sum(direction, [zero] + direction, -1.0)
        residual = polynomial_sum(residual, image, -step)
        if iteration + 1 < ITERS:
            fresh = inner(residual, residual, moments)
            direction = polynomial_sum(residual, direction, fresh / energy)
            energy = fresh
    return pressure, residual


def kernel(
    sizes, groups, right_hbm, mask_hbm, pressure_ref, scaled_ref,
    right_ref, mask_ref, fields, phases, coefs, diag, sz0, sx0, rz0, rx0, sx, sy, rz, rx, ry,
    partial, gathered, load_sems, send_sems, recv_sems, sum_send, sum_recv,
):
    depth, rows, lanes = right_ref.shape
    peers = []
    for offset in [dict([(a, o)]) for a in AXES for o in (1, sizes[a] - 1)] + [
        o for group in groups for o in group_offsets(sizes, group)
    ]:
        if offset not in peers:
            peers.append(offset)
    barrier = pltpu.get_barrier_semaphore()
    for offset in peers:
        pl.semaphore_signal(barrier, inc=1, device_id=shifted(sizes, offset), device_id_type=MESH)
    loads = [
        pltpu.make_async_copy(mask_hbm, mask_ref, load_sems.at[0]),
        pltpu.make_async_copy(right_hbm, right_ref, load_sems.at[1]),
    ]
    for load in loads:
        load.start()

    row = lax.broadcasted_iota(jnp.int32, (rows, lanes), 0)
    lane = lax.broadcasted_iota(jnp.int32, (rows, lanes), 1)
    even = lane % 2 == 0

    def pack(packed, plane, z, base):
        at = base + 2 * z
        turned = pltpu.roll(plane, (at + 1) % lanes, 1)
        return jnp.where((lane == at) | (lane == at + 1), turned, packed)

    def unpack(below, above):
        return jnp.where(even, pltpu.roll(above, lanes - 1, 1), pltpu.roll(below, 1, 1))

    def neighbours(plane, under, over, low_row, high_row, sides, z, base):
        at = base + 2 * z
        edge = pltpu.roll(sides, (lanes - at - 1) % lanes, 1)
        return (
            under,
            over,
            jnp.where(row == 0, low_row, pltpu.roll(plane, 1, 0)),
            jnp.where(row == rows - 1, high_row, pltpu.roll(plane, rows - 1, 0)),
            jnp.where(lane == 0, edge, pltpu.roll(plane, 1, 1)),
            jnp.where(lane == lanes - 1, edge, pltpu.roll(plane, lanes - 1, 1)),
        )

    for load in loads:
        load.wait()
    for side, z in ((0, 0), (1, depth - 1)):
        sz0[side, 0] = right_ref[z]
        sz0[side, 1] = mask_ref[z].astype(F32).astype(jnp.bfloat16)
    pl.semaphore_wait(barrier, len(peers))
    z_copies = exchange(
        sizes, 0, "gz", (sz0.at[0], sz0.at[1]), (rz0.at[0], rz0.at[1]), send_sems, recv_sems
    )
    packed = jnp.zeros((rows, lanes), F32)
    for z in range(depth):
        value = right_ref[z].astype(F32)
        phase = mask_ref[z].astype(F32)
        fields[0, z] = value
        phases[z] = phase
        packed = pack(packed, value, z, 0)
        packed = pack(packed, phase, z, 2 * depth)
        for part, plane in enumerate((value, phase)):
            sx0[0, part, z : z + 1, :] = plane[0:1]
            sx0[1, part, z : z + 1, :] = plane[rows - 1 : rows]
    sy[0] = packed
    y_copies = exchange(
        sizes, 0, "gy", (sy.at[0], sy.at[0]), (ry.at[0, 0], ry.at[0, 1]), send_sems, recv_sems
    )
    x_copies = exchange(
        sizes, 0, "gx", (sx0.at[0], sx0.at[1]), (rx0.at[0], rx0.at[1]), send_sems, recv_sems
    )

    def fold(product):
        return jnp.sum(product.reshape(rows // 8, 8, lanes), axis=0)

    sums = [jnp.zeros((8, lanes), F32) for _ in range(2 * ITERS)]
    mixed = 2.0 / (density_gas + density_liquid)
    inner = list(range(1, depth - 1))
    for phase in range(ITERS):
        for copy in y_copies + x_copies:
            copy.wait()
        sides = unpack(ry[phase, 0], ry[phase, 1])
        packed = jnp.zeros((rows, lanes), F32)
        for z in inner + [0, depth - 1]:
            if z == 0:
                for copy in z_copies:
                    copy.wait()
            if phase == 0:
                below = rz0[0, 1].astype(F32) if z == 0 else phases[z - 1]
                above = rz0[1, 1].astype(F32) if z == depth - 1 else phases[z + 1]
                own = phases[z]
                around = neighbours(
                    own, below, above,
                    rx0[0, 1, z : z + 1, :], rx0[1, 1, z : z + 1, :], sides, z, 2 * depth,
                )
                weights = []
                diagonal = jnp.full((rows, lanes), mass_shift, F32)
                for other in around:
                    count = own + other
                    weight = jnp.where(
                        count < 0.5,
                        1.0 / density_gas,
                        jnp.where(count < 1.5, mixed, 1.0 / density_liquid),
                    )
                    weights.append(weight)
                    diagonal = diagonal + weight
                diag[z] = diagonal
                inverse = 1.0 / diagonal
                weights = [weight * inverse for weight in weights]
                for k, weight in enumerate(weights):
                    coefs[k, z] = weight
                below = rz0[0, 0].astype(F32) if z == 0 else fields[0, z - 1]
                above = rz0[1, 0].astype(F32) if z == depth - 1 else fields[0, z + 1]
                low, high = rx0[0, 0, z : z + 1, :], rx0[1, 0, z : z + 1, :]
            else:
                diagonal = diag[z]
                weights = [coefs[k, z] for k in range(6)]
                below = rz[phase - 1, 0] if z == 0 else fields[phase, z - 1]
                above = rz[phase - 1, 1] if z == depth - 1 else fields[phase, z + 1]
                low, high = rx[phase - 1, 0, z : z + 1, :], rx[phase - 1, 1, z : z + 1, :]
            own = fields[phase, z]
            around = neighbours(own, below, above, low, high, sides, z, 0)
            mean = weights[0] * around[0]
            for weight, other in zip(weights[1:], around[1:]):
                mean = mean + weight * other
            fields[phase + 1, z] = mean
            scaled = diagonal * own
            sums[2 * phase] = sums[2 * phase] + fold(scaled * own)
            sums[2 * phase + 1] = sums[2 * phase + 1] + fold(scaled * mean)
            if phase + 1 < ITERS:
                packed = pack(packed, mean, z, 0)
                sx[phase, 0, z : z + 1, :] = mean[0:1]
                sx[phase, 1, z : z + 1, :] = mean[rows - 1 : rows]
        if phase + 1 < ITERS:
            z_copies = exchange(
                sizes, phase + 1, "gz",
                (fields.at[phase + 1, 0], fields.at[phase + 1, depth - 1]),
                (rz.at[phase, 0], rz.at[phase, 1]),
                send_sems, recv_sems,
            )
            sy[phase + 1] = packed
            y_copies = exchange(
                sizes, phase + 1, "gy",
                (sy.at[phase + 1], sy.at[phase + 1]),
                (ry.at[phase + 1, 0], ry.at[phase + 1, 1]),
                send_sems, recv_sems,
            )
            x_copies = exchange(
                sizes, phase + 1, "gx",
                (sx.at[phase, 0], sx.at[phase, 1]),
                (rx.at[phase, 0], rx.at[phase, 1]),
                send_sems, recv_sems,
            )

    place = lax.broadcasted_iota(jnp.int32, (1, lanes), 1)
    tile = jnp.zeros((1, lanes), F32)
    for k, total in enumerate(sums):
        line = jnp.sum(total, axis=0, keepdims=True)
        tile = jnp.where(place == k, jnp.sum(line, axis=1, keepdims=True), tile)
    slot = 0
    for number, group in enumerate(groups):
        partial[number] = tile
        copies = []
        first = slot
        for offset in group_offsets(sizes, group):
            copy = pltpu.make_async_remote_copy(
                src_ref=partial.at[number],
                dst_ref=gathered.at[slot],
                send_sem=sum_send.at[slot],
                recv_sem=sum_recv.at[slot],
                device_id=shifted(sizes, offset),
                device_id_type=MESH,
            )
            copy.start()
            copies.append(copy)
            slot += 1
        for copy in copies:
            copy.wait()
        for k in range(first, slot):
            tile = tile + gathered[k]

    moments = [tile[:, k : k + 1] for k in range(2 * ITERS)]
    pressure, residual = gradient_coefficients(moments)
    for z in range(depth):
        basis = [fields[k, z] for k in range(ITERS + 1)]
        for ref, factors in ((pressure_ref, pressure), (scaled_ref, residual)):
            total = factors[0] * basis[0]
            for factor, part in zip(factors[1:], basis[1:]):
                total = total + factor * part
            ref[z] = total


def choose_groups(sizes, most=32):
    groups = []
    for axis in ("gz", "gy", "gx"):
        if groups and sizes[axis] * functools.reduce(lambda n, a: n * sizes[a], groups[-1], 1) <= most:
            groups[-1] = groups[-1] + (axis,)
        else:
            groups.append((axis,))
    return tuple(groups)


def solution(mesh):
    sizes = {axis: mesh.shape[axis] for axis in AXES}
    groups = choose_groups(sizes, 32)
    slots = sum(len(group_offsets(sizes, group)) for group in groups)

    def on_device(right_side, phase_mask):
        depth, rows, lanes = right_side.shape
        block = jax.ShapeDtypeStruct((depth, rows, lanes), F32)
        face = (rows, lanes)
        return pl.pallas_call(
            functools.partial(kernel, sizes, groups),
            out_shape=(block, block),
            in_specs=[pl.BlockSpec(memory_space=pltpu.HBM)] * 2,
            out_specs=(pl.BlockSpec(memory_space=pltpu.VMEM),) * 2,
            scratch_shapes=[
                pltpu.VMEM((depth, *face), jnp.bfloat16),
                pltpu.VMEM((depth, *face), jnp.int32),
                pltpu.VMEM((ITERS + 1, depth, *face), F32),
                pltpu.VMEM((depth, *face), F32),
                pltpu.VMEM((6, depth, *face), F32),
                pltpu.VMEM((depth, *face), F32),
                pltpu.VMEM((2, 2, *face), jnp.bfloat16),
                pltpu.VMEM((2, 2, depth, lanes), F32),
                pltpu.VMEM((2, 2, *face), jnp.bfloat16),
                pltpu.VMEM((2, 2, depth, lanes), F32),
                pltpu.VMEM((ITERS - 1, 2, depth, lanes), F32),
                pltpu.VMEM((ITERS, *face), F32),
                pltpu.VMEM((ITERS - 1, 2, *face), F32),
                pltpu.VMEM((ITERS - 1, 2, depth, lanes), F32),
                pltpu.VMEM((ITERS, 2, *face), F32),
                pltpu.VMEM((len(groups), 1, lanes), F32),
                pltpu.VMEM((slots, 1, lanes), F32),
                pltpu.SemaphoreType.DMA((2,)),
                pltpu.SemaphoreType.DMA((ITERS, 6)),
                pltpu.SemaphoreType.DMA((ITERS, 6)),
                pltpu.SemaphoreType.DMA((slots,)),
                pltpu.SemaphoreType.DMA((slots,)),
            ],
            compiler_params=pltpu.CompilerParams(collective_id=0, has_side_effects=True, vmem_limit_bytes=16 * 2**20),
        )(right_side, phase_mask)

    return jax.shard_map(
        on_device,
        mesh=mesh,
        in_specs=(P("gz", "gx", "gy"), P("gz", "gx", "gy")),
        out_specs=(P("gz", "gx", "gy"), P("gz", "gx", "gy")),
        check_vma=False,
    )
```

```python
import functools
import itertools

import jax
import jax.numpy as jnp
from jax import lax
from jax.experimental import pallas as pl
from jax.experimental.pallas import tpu as pltpu
from jax.sharding import PartitionSpec as P

ITERS = 3
AXES = ("gx", "gy", "gz")
MESH = pl.DeviceIdType.MESH
F32 = jnp.float32

density_gas = 1.0
density_liquid = 1000.0
mass_shift = 0.05


def shifted(sizes, offsets):
    return {
        axis: lax.rem(lax.axis_index(axis) + offset, sizes[axis])
        for axis, offset in offsets.items()
        if offset
    }


def group_offsets(sizes, group):
    spans = [range(sizes[axis]) for axis in group]
    return [dict(zip(group, point)) for point in itertools.product(*spans) if any(point)]


def exchange(sizes, phase, axis, faces, landings, send_sems, recv_sems):
    place = AXES.index(axis)
    copies = []
    for side, offset in ((0, 1), (1, sizes[axis] - 1)):
        copy = pltpu.make_async_remote_copy(
            src_ref=faces[1 - side],
            dst_ref=landings[side],
            send_sem=send_sems.at[phase, 2 * place + side],
            recv_sem=recv_sems.at[phase, 2 * place + side],
            device_id=shifted(sizes, {axis: offset}),
            device_id_type=MESH,
        )
        copy.start()
        copies.append(copy)
    return copies


def polynomial_sum(first, second, factor):
    length = max(len(first), len(second))
    out = []
    for i in range(length):
        if i >= len(second):
            out.append(first[i])
        elif i >= len(first):
            out.append(factor * second[i])
        else:
            out.append(first[i] + factor * second[i])
    return out


def gradient_coefficients(moments):
    one, zero = jnp.ones_like(moments[0]), jnp.zeros_like(moments[0])

    def inner(first, second, weights):
        total = None
        for i, a in enumerate(first):
            for j, b in enumerate(second):
                term = a * b * weights[i + j]
                total = term if total is None else total + term
        return total

    drops = [moments[i] - moments[i + 1] for i in range(len(moments) - 1)]
    residual, direction, pressure = [one], [one], []
    energy = moments[0]
    for iteration in range(ITERS):
        step = energy / inner(direction, direction, drops)
        pressure = polynomial_sum(pressure, direction, step)
        image = polynomial_sum(direction, [zero] + direction, -1.0)
        residual = polynomial_sum(residual, image, -step)
        if iteration + 1 < ITERS:
            fresh = inner(residual, residual, moments)
            direction = polynomial_sum(residual, direction, fresh / energy)
            energy = fresh
    return pressure, residual


def kernel(
    sizes, groups, right_hbm, mask_hbm, pressure_ref, scaled_ref,
    right_ref, mask_ref, fields, phases, coefs, diag, sz0, sx0, rz0, rx0, sx, sy, rz, rx, ry,
    partial, gathered, load_sems, send_sems, recv_sems, sum_send, sum_recv,
):
    depth, rows, lanes = right_ref.shape
    peers = []
    for offset in [dict([(a, o)]) for a in AXES for o in (1, sizes[a] - 1)] + [
        o for group in groups for o in group_offsets(sizes, group)
    ]:
        if offset not in peers:
            peers.append(offset)
    barrier = pltpu.get_barrier_semaphore()
    for offset in peers:
        pl.semaphore_signal(barrier, inc=1, device_id=shifted(sizes, offset), device_id_type=MESH)
    loads = [
        pltpu.make_async_copy(mask_hbm, mask_ref, load_sems.at[0]),
        pltpu.make_async_copy(right_hbm, right_ref, load_sems.at[1]),
    ]
    for load in loads:
        load.start()

    row = lax.broadcasted_iota(jnp.int32, (rows, lanes), 0)
    lane = lax.broadcasted_iota(jnp.int32, (rows, lanes), 1)
    even = lane % 2 == 0

    def pack(packed, plane, z, base):
        at = base + 2 * z
        turned = pltpu.roll(plane, (at + 1) % lanes, 1)
        return jnp.where((lane == at) | (lane == at + 1), turned, packed)

    def unpack(below, above):
        return jnp.where(even, pltpu.roll(above, lanes - 1, 1), pltpu.roll(below, 1, 1))

    def neighbours(plane, under, over, low_row, high_row, sides, z, base):
        at = base + 2 * z
        edge = pltpu.roll(sides, (lanes - at - 1) % lanes, 1)
        return (
            under,
            over,
            jnp.where(row == 0, low_row, pltpu.roll(plane, 1, 0)),
            jnp.where(row == rows - 1, high_row, pltpu.roll(plane, rows - 1, 0)),
            jnp.where(lane == 0, edge, pltpu.roll(plane, 1, 1)),
            jnp.where(lane == lanes - 1, edge, pltpu.roll(plane, lanes - 1, 1)),
        )

    for load in loads:
        load.wait()
    for side, z in ((0, 0), (1, depth - 1)):
        sz0[side, 0] = right_ref[z]
        sz0[side, 1] = mask_ref[z].astype(F32).astype(jnp.bfloat16)
    pl.semaphore_wait(barrier, len(peers))
    z_copies = exchange(
        sizes, 0, "gz", (sz0.at[0], sz0.at[1]), (rz0.at[0], rz0.at[1]), send_sems, recv_sems
    )
    packed = jnp.zeros((rows, lanes), F32)
    for z in range(depth):
        value = right_ref[z].astype(F32)
        phase = mask_ref[z].astype(F32)
        fields[0, z] = value
        phases[z] = phase
        packed = pack(packed, value, z, 0)
        packed = pack(packed, phase, z, 2 * depth)
        for part, plane in enumerate((value, phase)):
            sx0[0, part, z : z + 1, :] = plane[0:1]
            sx0[1, part, z : z + 1, :] = plane[rows - 1 : rows]
    sy[0] = packed
    y_copies = exchange(
        sizes, 0, "gy", (sy.at[0], sy.at[0]), (ry.at[0, 0], ry.at[0, 1]), send_sems, recv_sems
    )
    x_copies = exchange(
        sizes, 0, "gx", (sx0.at[0], sx0.at[1]), (rx0.at[0], rx0.at[1]), send_sems, recv_sems
    )

    def fold(product):
        return jnp.sum(product.reshape(rows // 8, 8, lanes), axis=0)

    sums = [jnp.zeros((8, lanes), F32) for _ in range(2 * ITERS)]
    mixed = 2.0 / (density_gas + density_liquid)
    inner = list(range(1, depth - 1))
    for phase in range(ITERS):
        for copy in y_copies + x_copies:
            copy.wait()
        sides = unpack(ry[phase, 0], ry[phase, 1])
        packed = jnp.zeros((rows, lanes), F32)
        for z in inner + [0, depth - 1]:
            if z == 0:
                for copy in z_copies:
                    copy.wait()
            if phase == 0:
                below = rz0[0, 1].astype(F32) if z == 0 else phases[z - 1]
                above = rz0[1, 1].astype(F32) if z == depth - 1 else phases[z + 1]
                own = phases[z]
                around = neighbours(
                    own, below, above,
                    rx0[0, 1, z : z + 1, :], rx0[1, 1, z : z + 1, :], sides, z, 2 * depth,
                )
                weights = []
                diagonal = jnp.full((rows, lanes), mass_shift, F32)
                for other in around:
                    count = own + other
                    weight = jnp.where(
                        count < 0.5,
                        1.0 / density_gas,
                        jnp.where(count < 1.5, mixed, 1.0 / density_liquid),
                    )
                    weights.append(weight)
                    diagonal = diagonal + weight
                diag[z] = diagonal
                inverse = 1.0 / diagonal
                weights = [weight * inverse for weight in weights]
                for k, weight in enumerate(weights):
                    coefs[k, z] = weight
                below = rz0[0, 0].astype(F32) if z == 0 else fields[0, z - 1]
                above = rz0[1, 0].astype(F32) if z == depth - 1 else fields[0, z + 1]
                low, high = rx0[0, 0, z : z + 1, :], rx0[1, 0, z : z + 1, :]
            else:
                diagonal = diag[z]
                weights = [coefs[k, z] for k in range(6)]
                below = rz[phase - 1, 0] if z == 0 else fields[phase, z - 1]
                above = rz[phase - 1, 1] if z == depth - 1 else fields[phase, z + 1]
                low, high = rx[phase - 1, 0, z : z + 1, :], rx[phase - 1, 1, z : z + 1, :]
            own = fields[phase, z]
            around = neighbours(own, below, above, low, high, sides, z, 0)
            mean = weights[0] * around[0]
            for weight, other in zip(weights[1:], around[1:]):
                mean = mean + weight * other
            fields[phase + 1, z] = mean
            scaled = diagonal * own
            sums[2 * phase] = sums[2 * phase] + fold(scaled * own)
            sums[2 * phase + 1] = sums[2 * phase + 1] + fold(scaled * mean)
            if phase + 1 < ITERS:
                packed = pack(packed, mean, z, 0)
                sx[phase, 0, z : z + 1, :] = mean[0:1]
                sx[phase, 1, z : z + 1, :] = mean[rows - 1 : rows]
        if phase + 1 < ITERS:
            z_copies = exchange(
                sizes, phase + 1, "gz",
                (fields.at[phase + 1, 0], fields.at[phase + 1, depth - 1]),
                (rz.at[phase, 0], rz.at[phase, 1]),
                send_sems, recv_sems,
            )
            sy[phase + 1] = packed
            y_copies = exchange(
                sizes, phase + 1, "gy",
                (sy.at[phase + 1], sy.at[phase + 1]),
                (ry.at[phase + 1, 0], ry.at[phase + 1, 1]),
                send_sems, recv_sems,
            )
            x_copies = exchange(
                sizes, phase + 1, "gx",
                (sx.at[phase, 0], sx.at[phase, 1]),
                (rx.at[phase, 0], rx.at[phase, 1]),
                send_sems, recv_sems,
            )

    place = lax.broadcasted_iota(jnp.int32, (1, lanes), 1)
    tile = jnp.zeros((1, lanes), F32)
    for k, total in enumerate(sums):
        line = jnp.sum(total, axis=0, keepdims=True)
        tile = jnp.where(place == k, jnp.sum(line, axis=1, keepdims=True), tile)
    slot = 0
    for number, group in enumerate(groups):
        partial[number] = tile
        copies = []
        first = slot
        for offset in group_offsets(sizes, group):
            copy = pltpu.make_async_remote_copy(
                src_ref=partial.at[number],
                dst_ref=gathered.at[slot],
                send_sem=sum_send.at[slot],
                recv_sem=sum_recv.at[slot],
                device_id=shifted(sizes, offset),
                device_id_type=MESH,
            )
            copy.start()
            copies.append(copy)
            slot += 1
        for copy in copies:
            copy.wait()
        for k in range(first, slot):
            tile = tile + gathered[k]

    moments = [tile[:, k : k + 1] for k in range(2 * ITERS)]
    pressure, residual = gradient_coefficients(moments)
    for z in range(depth):
        basis = [fields[k, z] for k in range(ITERS + 1)]
        for ref, factors in ((pressure_ref, pressure), (scaled_ref, residual)):
            total = factors[0] * basis[0]
            for factor, part in zip(factors[1:], basis[1:]):
                total = total + factor * part
            ref[z] = total


def choose_groups(sizes, most=32):
    groups = []
    for axis in ("gz", "gy", "gx"):
        if groups and sizes[axis] * functools.reduce(lambda n, a: n * sizes[a], groups[-1], 1) <= most:
            groups[-1] = groups[-1] + (axis,)
        else:
            groups.append((axis,))
    return tuple(groups)


def solution(mesh):
    sizes = {axis: mesh.shape[axis] for axis in AXES}
    groups = choose_groups(sizes, 32)
    slots = sum(len(group_offsets(sizes, group)) for group in groups)

    def on_device(right_side, phase_mask):
        depth, rows, lanes = right_side.shape
        block = jax.ShapeDtypeStruct((depth, rows, lanes), F32)
        face = (rows, lanes)
        return pl.pallas_call(
            functools.partial(kernel, sizes, groups),
            out_shape=(block, block),
            in_specs=[pl.BlockSpec(memory_space=pltpu.HBM)] * 2,
            out_specs=(pl.BlockSpec(memory_space=pltpu.VMEM),) * 2,
            scratch_shapes=[
                pltpu.VMEM((depth, *face), jnp.bfloat16),
                pltpu.VMEM((depth, *face), jnp.int32),
                pltpu.VMEM((ITERS + 1, depth, *face), F32),
                pltpu.VMEM((depth, *face), F32),
                pltpu.VMEM((6, depth, *face), F32),
                pltpu.VMEM((depth, *face), F32),
                pltpu.VMEM((2, 2, *face), jnp.bfloat16),
                pltpu.VMEM((2, 2, depth, lanes), F32),
                pltpu.VMEM((2, 2, *face), jnp.bfloat16),
                pltpu.VMEM((2, 2, depth, lanes), F32),
                pltpu.VMEM((ITERS - 1, 2, depth, lanes), F32),
                pltpu.VMEM((ITERS, *face), F32),
                pltpu.VMEM((ITERS - 1, 2, *face), F32),
                pltpu.VMEM((ITERS - 1, 2, depth, lanes), F32),
                pltpu.VMEM((ITERS, 2, *face), F32),
                pltpu.VMEM((len(groups), 1, lanes), F32),
                pltpu.VMEM((slots, 1, lanes), F32),
                pltpu.SemaphoreType.DMA((2,)),
                pltpu.SemaphoreType.DMA((ITERS, 6)),
                pltpu.SemaphoreType.DMA((ITERS, 6)),
                pltpu.SemaphoreType.DMA((slots,)),
                pltpu.SemaphoreType.DMA((slots,)),
            ],
            compiler_params=pltpu.CompilerParams(collective_id=0, has_side_effects=True, vmem_limit_bytes=54408 * 2**10),
        )(right_side, phase_mask)

    return jax.shard_map(
        on_device,
        mesh=mesh,
        in_specs=(P("gz", "gx", "gy"), P("gz", "gx", "gy")),
        out_specs=(P("gz", "gx", "gy"), P("gz", "gx", "gy")),
        check_vma=False,
    )
```
